32 devices in a mesh: dp: 8 (over z, x), vocab: 4 (over y, core).
Axes of the slice: x: 2, y: 2, z: 4, core: 2. Of those that a mesh axis runs over, the one named last changes fastest.
Arguments:
- hidden_states: bfloat16 [1024, 3584], P('dp', 'vocab'), may hold values from -750 to 750, as said below
- head_weight: bfloat16 [152064, 3584], P(('dp', 'vocab')), may hold values from -0.09375 to 0.09375
- token_ids: int32 [1024], P('dp'), may hold values from 0 to 152063
- response_mask: int32 [1024], P('dp'), may hold values 0 or 1
- rollout_logprobs: float32 [1024], P('dp'), may hold values from -14 to -6
- advantages: float32 [1024], P('dp'), may hold values from -6 to 6
Outputs:
- logprobs: float32 [1024], P('dp')
- tis_weight: float32 [1024], P('dp')
- loss: float32 [], replicated
The draws below stay inside these ranges and needn't reach their ends.
Inputs may be any that keep to these rules, and one draw needn't show every extreme that they name: `hidden_states`: hidden states; some rows may be far larger than others.
All inputs are finite; a program needn't handle non-finite values. No bound on the sum of `response_mask` on one device may be relied on, other than what follows from the above.
Results may differ from the reference program's by a relative error of at most 0.0003.
Values may be sent and summed in bfloat16 or wider, within the bound.
A program may use at most 128 MiB of HBM per device.

```python
import jax
import jax.numpy as jnp
from jax import lax

D = 3584
VOCAB = 152064
LENGTH = 128
TOKENS = 1024


def draw_hidden_states(key, part):
    base = jnp.clip(jax.random.normal(jax.random.fold_in(key, 11), (TOKENS, D), jnp.float32), -5.0, 5.0)
    return base.astype(jnp.bfloat16)


def place_ends(result, own_key, low, top_value):
    place = [jax.random.randint(jax.random.fold_in(own_key, axis), (), 0, length) for axis, length in enumerate(result.shape)]
    main_axis = result.shape.index(max(result.shape))
    beside = place[:main_axis] + [(place[main_axis] + 1) % result.shape[main_axis]] + place[main_axis + 1:]
    return result.at[tuple(place)].set(low).at[tuple(beside)].set(top_value)


def steps_of(own_key, extent, cuts, least, largest):
    level = 1.0
    for position, blocks in cuts:
        draws = jax.random.uniform(jax.random.fold_in(jax.random.fold_in(own_key, 6), position), (blocks,), jnp.float32, least / len(cuts), largest / len(cuts))
        level = level * jnp.repeat(jnp.exp(draws), extent[position] // blocks).reshape((-1,) + (1,) * (len(extent) - 1 - position))
    return level


def gaussian(own_key, extent, spread, limit, pieces=(), held_as=jnp.bfloat16):
    entries = spread * jax.random.normal(own_key, extent, jnp.float32)
    if pieces:
        entries = entries * steps_of(own_key, extent, pieces, -0.22, 0.18)
    return jnp.clip(entries, -limit, limit).astype(held_as)


def setup_inputs(seed: int = 0) -> dict:
    splits = jax.random.split(jax.random.key(seed), 7)
    return {
        "hidden_states": draw_hidden_states(jax.random.fold_in(splits[6], 71), 0),
        "head_weight": gaussian(splits[1], (VOCAB, D), D ** -0.5, 0.09375, ((0, 32),)),
        "token_ids": place_ends(jax.random.randint(splits[2], (TOKENS,), 0, VOCAB), jax.random.fold_in(splits[2], 1), 0, VOCAB - 1).astype(jnp.int32),
        "response_mask": place_ends((jax.random.randint(splits[3], (TOKENS,), 0, 4) < 3).astype(jnp.int32), jax.random.fold_in(splits[3], 1), 0, 1),
        "rollout_logprobs": jnp.clip(-14.0 + 8.0 * jax.random.uniform(splits[4], (TOKENS,), jnp.float32) ** steps_of(splits[4], (TOKENS,), ((0, 8),), -0.2, 0.2), -14.0, -6.0),
        "advantages": gaussian(splits[5], (TOKENS,), 1.0, 6.0, ((0, 8),), jnp.float32),
    }


def reference(hidden_states, head_weight, token_ids, response_mask, rollout_logprobs, advantages):
    def block_logprobs(items):
        rows, ids = items
        logits = jnp.dot(rows, head_weight.T, preferred_element_type=jnp.float32)
        top = jnp.max(logits, axis=1)
        lse = top + jnp.log(jnp.sum(jnp.exp(logits - top[:, None]), axis=1))
        picked = jnp.take_along_axis(logits, ids[:, None].astype(jnp.int32), axis=1)[:, 0]
        return picked - lse

    blocks = hidden_states.reshape(-1, LENGTH, D)
    id_blocks = token_ids.reshape(-1, LENGTH)
    logprobs = lax.map(block_logprobs, (blocks, id_blocks)).reshape(-1)
    tis_weight = jnp.minimum(jnp.exp(logprobs - rollout_logprobs), 2.0)
    counted = response_mask.astype(jnp.float32)
    count = jnp.sum(counted)
    loss = -jnp.sum(counted * tis_weight * advantages * logprobs) / jnp.maximum(count, 1.0)
    return logprobs, tis_weight, loss
```

```python
import functools

import jax
import jax.numpy as jnp
from jax import lax
from jax.experimental import pallas as pl
from jax.experimental.pallas import tpu as pltpu
from jax.sharding import PartitionSpec as P

MESH = pl.DeviceIdType.MESH
VMEM_BYTES = 64000 * 1024
LOW = -3.0e38


def shard_stats(logits, ids_block, columns):
    matched = columns[None, :] == ids_block[:, None]
    picked = jnp.sum(jnp.where(matched, logits, 0.0), axis=1)
    peak = jnp.max(logits, axis=1)
    total = jnp.sum(jnp.exp(logits - peak[:, None]), axis=1)
    return (peak, total, picked)


def token_terms(logp, rollout, advant, mask):
    weight = jnp.minimum(jnp.exp(logp - rollout), 2.0)
    counted = mask.astype(jnp.float32)
    loss_part = -jnp.sum(counted * weight * advant * logp)
    return (weight, loss_part, jnp.sum(counted))


def general_body(hidden_states, head_weight, token_ids, response_mask, rollout_logprobs, advantages):
    rows_local = token_ids.shape[0]
    vocab_local = head_weight.shape[0]
    offset = lax.axis_index(("dp", "vocab")) * vocab_local
    own_columns = lax.iota(jnp.int32, vocab_local) + offset
    own_start = lax.axis_index("dp") * rows_local
    gather = functools.partial(lax.all_gather, axis_name="dp", axis=0, tiled=True)
    all_ids, all_mask = gather(token_ids), gather(response_mask)
    all_rollout, all_advant = gather(rollout_logprobs), gather(advantages)
    full_rows = lax.all_gather(hidden_states, "vocab", axis=1, tiled=True)
    logits = jnp.einsum("rd,vd->rv", gather(full_rows), head_weight, preferred_element_type=jnp.float32)
    peak, total, picked = shard_stats(logits, all_ids, own_columns)
    top = lax.pmax(peak, ("dp", "vocab"))
    total_sum, picked_sum = lax.psum((total * jnp.exp(peak - top), picked), ("dp", "vocab"))
    logprob_all = picked_sum - (top + jnp.log(total_sum))
    own_logp = lax.dynamic_slice_in_dim(logprob_all, own_start, rows_local, 0)
    weight_all, loss_sum, count = token_terms(logprob_all, all_rollout, all_advant, all_mask)
    weight = lax.dynamic_slice_in_dim(weight_all, own_start, rows_local, 0)
    return (own_logp, weight, loss_sum / jnp.maximum(count, 1.0))


L, XA, XB, YA, YB, D0, D1, PL, PX, PY, PD = range(11)


def kernel(dp, nv, rows, feats, vt, tiles, x_hbm, w_hbm, side_ref, out_ref,
           h_ref, w_ref, logit_ref, m_ref, l_ref, p_ref, stat_ref, side_buf, fin_ref,
           recv, send, wsem, own_sem, side_recv, side_send, stat_recv, stat_send):
    chunks = dp // 2
    half = rows // 2
    cols = 2 * rows
    everyone = dp * nv
    g_me, v_me = lax.axis_index("dp"), lax.axis_index("vocab")
    me = g_me * nv + v_me
    z, x, y, k = g_me // 2, g_me % 2, v_me // 2, v_me % 2
    xn, yn, kn = 1 - x, 1 - y, 1 - k
    to_x = (g_me + 1 - 2 * x, v_me)
    to_y = (g_me, yn * 2 + k)
    to_p = (g_me, y * 2 + kn)
    to_z = ((g_me + 2) % dp, v_me)

    def wcopy(i):
        return pltpu.make_async_copy(w_hbm.at[pl.ds(pl.multiple_of(i * vt, 16), vt)], w_ref.at[i], wsem.at[i])

    def block(c, bx, by, bk, first=0, count=rows):
        return h_ref.at[c, pl.ds(pl.multiple_of(bx * rows + first, 16), count),
                        pl.ds(pl.multiple_of((by * 2 + bk) * feats, 128), feats)]

    own = block(z, x, y, k)
    own_copy = pltpu.make_async_copy(x_hbm, own, own_sem)
    own_copy.start()

    barrier = pltpu.get_barrier_semaphore()

    def greet(o, carry):
        t = (me + o) % everyone
        pl.semaphore_signal(barrier, inc=1, device_id=(t // nv, t % nv), device_id_type=MESH)
        return carry

    lax.fori_loop(1, everyone, greet, 0)
    lax.fori_loop(0, tiles, lambda i, a: (wcopy(i).start(), a)[1], 0)
    side_buf[g_me] = side_ref[...]
    own_copy.wait()
    pl.semaphore_wait(barrier, everyone - 1)

    def remote(ref, kind, t, to):
        return pltpu.make_async_remote_copy(
            src_ref=ref, dst_ref=ref, send_sem=send.at[kind, t], recv_sem=recv.at[kind, t],
            device_id=to, device_id_type=MESH)

    def came(ref, kind, t):
        pltpu.make_async_copy(ref, ref, recv.at[kind, t]).wait()

    def chunk_of(t):
        return (z - t + chunks) % chunks

    def line(t, wait):
        c = chunk_of(t)
        b = block(c, x, y, k)
        if wait:
            came(b, L, t)
        h0, h1 = block(c, x, y, k, 0, half), block(c, x, y, k, half, half)
        remote(h0, XA, t, to_x).start()
        remote(h1, YA, t, to_y).start()

        def onward():
            remote(b, L, t + 1, to_z).start()

        pl.when(t < chunks - 1)(onward)
        remote(h1, XB, t, to_x).start()
        remote(h0, YB, t, to_y).start()
        remote(b, PL, t, to_p).start()

    def relay(t):
        c = chunk_of(t)
        bx, by = block(c, xn, y, k, 0, half), block(c, x, yn, k, half, half)
        came(bx, XA, t)
        remote(bx, D0, t, to_y).start()
        came(by, YA, t)
        remote(by, D1, t, to_x).start()

    def across(t):
        c = chunk_of(t)
        came(block(c, xn, y, k, half, half), XB, t)
        remote(block(c, xn, y, k), PX, t, to_p).start()
        came(block(c, x, yn, k, 0, half), YB, t)
        remote(block(c, x, yn, k), PY, t, to_p).start()

    def corner(t):
        c = chunk_of(t)
        came(block(c, xn, yn, k, 0, half), D0, t)
        came(block(c, xn, yn, k, half, half), D1, t)
        remote(block(c, xn, yn, k), PD, t, to_p).start()

    def ready(t):
        c = chunk_of(t)
        came(block(c, x, y, kn), PL, t)
        came(block(c, xn, y, kn), PX, t)
        came(block(c, x, yn, kn), PY, t)
        came(block(c, xn, yn, kn), PD, t)

    line(0, False)

    def tell(o, carry):
        t = (g_me + o) % dp
        pltpu.make_async_remote_copy(
            src_ref=side_ref, dst_ref=side_buf.at[g_me], send_sem=side_send, recv_sem=side_recv,
            device_id=(t, v_me), device_id_type=MESH).start()
        return carry

    lax.fori_loop(1, dp, tell, 0)
    relay(0)
    if chunks > 1:
        line(1, True)
    across(0)
    corner(0)
    others = side_buf.at[pl.ds(0, dp - 1)]
    pltpu.make_async_copy(others, others, side_recv).wait()
    pltpu.make_async_copy(others, others, side_send).wait()
    logit_ref[1] = jnp.zeros((vt, cols), jnp.float32)

    sub = lax.broadcasted_iota(jnp.int32, (8, cols), 0)
    groups = vt // 8

    def epilogue(g):
        s, i = g // tiles, g % tiles
        slot = g % 2
        c = chunk_of(s)
        ids = jnp.concatenate([side_buf[2 * c, 0:1, :], side_buf[2 * c + 1, 0:1, :]], axis=1).astype(jnp.int32)
        rel = ids - (me * (vt * tiles) + i * vt) - sub
        first = jnp.full((8, cols), i, jnp.int32) == 0
        m_old = jnp.where(first, LOW, m_ref[...])
        tops = [m_old] + [None] * 3
        for j in range(groups):
            val = logit_ref[slot, 8 * j:8 * j + 8, :]
            q = j % 4
            tops[q] = val if tops[q] is None else jnp.maximum(tops[q], val)
        m_new = functools.reduce(jnp.maximum, [t for t in tops if t is not None])
        sums = [jnp.where(first, 0.0, l_ref[...]) * jnp.exp(m_old - m_new), jnp.zeros((8, cols), jnp.float32)]
        picks = [jnp.where(first, 0.0, p_ref[...]), jnp.zeros((8, cols), jnp.float32)]
        for j in range(groups):
            val = logit_ref[slot, 8 * j:8 * j + 8, :]
            q = j % 2
            sums[q] = sums[q] + jnp.exp(val - m_new)
            picks[q] = picks[q] + jnp.where(rel == 8 * j, val, 0.0)
        m_ref[...] = m_new
        l_ref[...] = sums[0] + sums[1]
        p_ref[...] = picks[0] + picks[1]

    def finish(s):
        c = chunk_of(s)
        m, l, p = m_ref[...], l_ref[...], p_ref[...]
        peak = jnp.max(m, axis=0, keepdims=True)
        total = jnp.sum(l * jnp.exp(m - peak), axis=0, keepdims=True)
        pick = jnp.sum(p, axis=0, keepdims=True)
        pad = jnp.zeros((2, rows), jnp.float32)
        stat_ref[me, c] = jnp.concatenate(
            [peak[:, :rows], peak[:, rows:], total[:, :rows], total[:, rows:],
             pick[:, :rows], pick[:, rows:], pad], axis=0)

    def spread(s):
        c = chunk_of(s)
        mine = stat_ref.at[me, c]

        def one(o, carry):
            t = (me + o) % everyone
            pltpu.make_async_remote_copy(
                src_ref=mine, dst_ref=mine, send_sem=stat_send, recv_sem=stat_recv,
                device_id=(t // nv, t % nv), device_id_type=MESH).start()
            return carry

        lax.fori_loop(1, everyone, one, 0)

    def step(g, carry):
        s, i = g // tiles, g % tiles
        slot = g % 2
        pl.when(s == 0)(lambda: wcopy(i).wait())
        pl.when(i == 0)(lambda: ready(s))

        def middle():
            relay(s + 1)
            pl.when(s + 2 < chunks)(lambda: line(s + 2, True))

        more = s + 1 < chunks
        pl.when((i == tiles // 3) & more)(middle)
        pl.when((i == (2 * tiles) // 3) & more)(lambda: across(s + 1))
        pl.when((i == tiles - 1) & more)(lambda: corner(s + 1))
        pl.when((i == 1) & (s > 0))(lambda: spread(s - 1))
        logit_ref[slot] = lax.dot_general(
            w_ref[i], h_ref[chunk_of(s)], (((1,), (1,)), ((), ())), preferred_element_type=jnp.float32)
        epilogue(jnp.where(g == 0, 1, g - 1))
        pl.when((i == 0) & (s > 0))(lambda: finish(s - 1))
        return carry

    last = chunks * tiles
    lax.fori_loop(0, last, step, 0)
    epilogue(last - 1)
    finish(chunks - 1)
    spread(chunks - 1)

    full, part = block(0, 0, 0, 0), block(0, 0, 0, 0, 0, half)

    def left(t, carry):
        for kind in (XA, XB, YA, YB, D0, D1):
            pltpu.make_async_copy(part, part, send.at[kind, t]).wait()
        for kind in (PL, PX, PY, PD):
            pltpu.make_async_copy(full, full, send.at[kind, t]).wait()
        pl.when(t > 0)(lambda: pltpu.make_async_copy(full, full, send.at[L, t]).wait())
        return carry

    lax.fori_loop(0, chunks, left, 0)
    rest = stat_ref.at[pl.ds(0, everyone - 1)]
    pltpu.make_async_copy(rest, rest, stat_recv).wait()
    pltpu.make_async_copy(rest, rest, stat_send).wait()

    loss_sum = jnp.zeros((1, rows), jnp.float32)
    count = jnp.zeros((1, rows), jnp.float32)
    for c in range(chunks):
        top = stat_ref[0, c]
        for d in range(1, everyone):
            top = jnp.maximum(top, stat_ref[d, c])
        total = jnp.zeros((2, rows), jnp.float32)
        pick = jnp.zeros((2, rows), jnp.float32)
        for d in range(everyone):
            t = stat_ref[d, c]
            total = total + t[2:4] * jnp.exp(t[0:2] - top[0:2])
            pick = pick + t[4:6]
        logp = pick - (top[0:2] + jnp.log(total))
        for r in range(2):
            g = 2 * c + r
            lp = logp[r:r + 1]
            mask, roll, adv = side_buf[g, 1:2, :], side_buf[g, 2:3, :], side_buf[g, 3:4, :]
            weight = jnp.minimum(jnp.exp(lp - roll), 2.0)
            loss_sum = loss_sum - mask * weight * adv * lp
            count = count + mask
            fin_ref[g, 0:1, :] = lp
            fin_ref[g, 1:2, :] = weight
    loss = jnp.sum(loss_sum, axis=1, keepdims=True) / jnp.maximum(jnp.sum(count, axis=1, keepdims=True), 1.0)
    out_ref[0:2, :] = fin_ref[g_me, 0:2, :]
    out_ref[2:8, :] = jnp.broadcast_to(loss, (6, rows))


def tile_rows(vocab_local):
    fits = [t for t in range(16, 545, 16) if vocab_local % t == 0]
    return max(fits) if fits else 0


def fused_body(dp, nv, vt, hidden_states, head_weight, token_ids, response_mask, rollout_logprobs, advantages):
    rows, feats = hidden_states.shape
    vocab_local, width = head_weight.shape
    chunks, tiles = dp // 2, vocab_local // vt
    side = jnp.stack([token_ids.astype(jnp.float32), response_mask.astype(jnp.float32),
                      rollout_logprobs, advantages] + [jnp.zeros_like(advantages)] * 4)
    any_spec = pl.BlockSpec(memory_space=pl.ANY)
    vmem_spec = pl.BlockSpec(memory_space=pltpu.VMEM)
    dma = pltpu.SemaphoreType.DMA
    out = pl.pallas_call(
        functools.partial(kernel, dp, nv, rows, feats, vt, tiles),
        out_shape=jax.ShapeDtypeStruct((8, rows), jnp.float32),
        in_specs=[any_spec, any_spec, vmem_spec],
        out_specs=vmem_spec,
        scratch_shapes=[
            pltpu.VMEM((chunks, 2 * rows, width), jnp.bfloat16),
            pltpu.VMEM((tiles, vt, width), jnp.bfloat16),
            pltpu.VMEM((2, vt, 2 * rows), jnp.float32),
            pltpu.VMEM((8, 2 * rows), jnp.float32),
            pltpu.VMEM((8, 2 * rows), jnp.float32),
            pltpu.VMEM((8, 2 * rows), jnp.float32),
            pltpu.VMEM((dp * nv, chunks, 8, rows), jnp.float32),
            pltpu.VMEM((dp, 8, rows), jnp.float32),
            pltpu.VMEM((dp, 8, rows), jnp.float32),
            dma((11, chunks)), dma((11, chunks)), dma((tiles,)), dma, dma, dma, dma, dma,
        ],
        compiler_params=pltpu.CompilerParams(
            collective_id=0, has_side_effects=True, vmem_limit_bytes=VMEM_BYTES),
    )(hidden_states, head_weight, side)
    return out[0], out[1], out[2, 0]


def solution(mesh):
    placed = (P("dp", "vocab"), P(("dp", "vocab"), None), P("dp"), P("dp"), P("dp"), P("dp"))
    dp, nv = mesh.shape["dp"], mesh.shape["vocab"]

    def body(hidden_states, head_weight, *rest):
        rows, feats = hidden_states.shape
        vt = tile_rows(head_weight.shape[0])
        held = 2 * (head_weight.size + rows * dp * head_weight.shape[1]) + 16 * vt * rows
        fits = (dp % 2 == 0 and dp > 2 and nv == 4 and vt > 0 and rows == 128 and feats % 128 == 0
                and held < VMEM_BYTES - (8 << 20))
        if fits:
            return fused_body(dp, nv, vt, hidden_states, head_weight, *rest)
        return general_body(hidden_states, head_weight, *rest)

    return jax.shard_map(
        body, mesh=mesh, in_specs=placed, out_specs=(P("dp"), P("dp"), P()), check_vma=False
    )
```

```python
import functools

import jax
import jax.numpy as jnp
from jax import lax
from jax.experimental import pallas as pl
from jax.experimental.pallas import tpu as pltpu
from jax.sharding import PartitionSpec as P

MESH = pl.DeviceIdType.MESH
VMEM_BYTES = 64000 * 1024
LOW = -3.0e38


def shard_stats(logits, ids_block, columns):
    matched = columns[None, :] == ids_block[:, None]
    picked = jnp.sum(jnp.where(matched, logits, 0.0), axis=1)
    peak = jnp.max(logits, axis=1)
    total = jnp.sum(jnp.exp(logits - peak[:, None]), axis=1)
    return (peak, total, picked)


def token_terms(logp, rollout, advant, mask):
    weight = jnp.minimum(jnp.exp(logp - rollout), 2.0)
    counted = mask.astype(jnp.float32)
    loss_part = -jnp.sum(counted * weight * advant * logp)
    return (weight, loss_part, jnp.sum(counted))


def general_body(hidden_states, head_weight, token_ids, response_mask, rollout_logprobs, advantages):
    rows_local = token_ids.shape[0]
    vocab_local = head_weight.shape[0]
    offset = lax.axis_index(("dp", "vocab")) * vocab_local
    own_columns = lax.iota(jnp.int32, vocab_local) + offset
    own_start = lax.axis_index("dp") * rows_local
    gather = functools.partial(lax.all_gather, axis_name="dp", axis=0, tiled=True)
    all_ids, all_mask = gather(token_ids), gather(response_mask)
    all_rollout, all_advant = gather(rollout_logprobs), gather(advantages)
    full_rows = lax.all_gather(hidden_states, "vocab", axis=1, tiled=True)
    logits = jnp.einsum("rd,vd->rv", gather(full_rows), head_weight, preferred_element_type=jnp.float32)
    peak, total, picked = shard_stats(logits, all_ids, own_columns)
    top = lax.pmax(peak, ("dp", "vocab"))
    total_sum, picked_sum = lax.psum((total * jnp.exp(peak - top), picked), ("dp", "vocab"))
    logprob_all = picked_sum - (top + jnp.log(total_sum))
    own_logp = lax.dynamic_slice_in_dim(logprob_all, own_start, rows_local, 0)
    weight_all, loss_sum, count = token_terms(logprob_all, all_rollout, all_advant, all_mask)
    weight = lax.dynamic_slice_in_dim(weight_all, own_start, rows_local, 0)
    return (own_logp, weight, loss_sum / jnp.maximum(count, 1.0))


L, XA, XB, YA, YB, D0, D1, PL, PX, PY, PD = range(11)


def kernel(dp, nv, rows, feats, vt, tiles, x_hbm, w_hbm, side_ref, out_ref,
           h_ref, w_ref, logit_ref, m_ref, l_ref, p_ref, stat_ref, side_buf, fin_ref,
           recv, send, wsem, own_sem, side_recv, side_send, stat_recv, stat_send):
    chunks = dp // 2
    half = rows // 2
    cols = 2 * rows
    everyone = dp * nv
    g_me, v_me = lax.axis_index("dp"), lax.axis_index("vocab")
    me = g_me * nv + v_me
    z, x, y, k = g_me // 2, g_me % 2, v_me // 2, v_me % 2
    xn, yn, kn = 1 - x, 1 - y, 1 - k
    to_x = (g_me + 1 - 2 * x, v_me)
    to_y = (g_me, yn * 2 + k)
    to_p = (g_me, y * 2 + kn)
    to_z = ((g_me + 2) % dp, v_me)

    def wcopy(i):
        return pltpu.make_async_copy(w_hbm.at[pl.ds(pl.multiple_of(i * vt, 16), vt)], w_ref.at[i], wsem.at[i])

    def block(c, bx, by, bk, first=0, count=rows):
        return h_ref.at[c, pl.ds(pl.multiple_of(bx * rows + first, 16), count),
                        pl.ds(pl.multiple_of((by * 2 + bk) * feats, 128), feats)]

    own = block(z, x, y, k)
    own_copy = pltpu.make_async_copy(x_hbm, own, own_sem)
    own_copy.start()

    barrier = pltpu.get_barrier_semaphore()

    def greet(o, carry):
        t = lax.rem(me + o, everyone)
        pl.semaphore_signal(barrier, inc=1, device_id=(lax.div(t, nv), lax.rem(t, nv)), device_id_type=MESH)
        return carry

    lax.fori_loop(1, everyone, greet, 0)
    lax.fori_loop(0, tiles, lambda i, a: (wcopy(i).start(), a)[1], 0)
    side_buf[g_me] = side_ref[...]
    own_copy.wait()
    pl.semaphore_wait(barrier, everyone - 1)

    def remote(ref, kind, t, to):
        return pltpu.make_async_remote_copy(
            src_ref=ref, dst_ref=ref, send_sem=send.at[kind, t], recv_sem=recv.at[kind, t],
            device_id=to, device_id_type=MESH)

    def came(ref, kind, t):
        pltpu.make_async_copy(ref, ref, recv.at[kind, t]).wait()

    def chunk_of(t):
        return (z - t + chunks) % chunks

    def line(t, wait):
        c = chunk_of(t)
        b = block(c, x, y, k)
        if wait:
            came(b, L, t)
        h0, h1 = block(c, x, y, k, 0, half), block(c, x, y, k, half, half)
        remote(h0, XA, t, to_x).start()
        remote(h1, YA, t, to_y).start()

        def onward():
            remote(b, L, t + 1, to_z).start()

        pl.when(t < chunks - 1)(onward)
        remote(h1, XB, t, to_x).start()
        remote(h0, YB, t, to_y).start()
        remote(b, PL, t, to_p).start()

    def relay(t):
        c = chunk_of(t)
        bx, by = block(c, xn, y, k, 0, half), block(c, x, yn, k, half, half)
        came(bx, XA, t)
        remote(bx, D0, t, to_y).start()
        came(by, YA, t)
        remote(by, D1, t, to_x).start()

    def across(t):
        c = chunk_of(t)
        came(block(c, xn, y, k, half, half), XB, t)
        remote(block(c, xn, y, k), PX, t, to_p).start()
        came(block(c, x, yn, k, 0, half), YB, t)
        remote(block(c, x, yn, k), PY, t, to_p).start()

    def corner(t):
        c = chunk_of(t)
        came(block(c, xn, yn, k, 0, half), D0, t)
        came(block(c, xn, yn, k, half, half), D1, t)
        remote(block(c, xn, yn, k), PD, t, to_p).start()

    def ready(t):
        c = chunk_of(t)
        came(block(c, x, y, kn), PL, t)
        came(block(c, xn, y, kn), PX, t)
        came(block(c, x, yn, kn), PY, t)
        came(block(c, xn, yn, kn), PD, t)

    line(0, False)

    def tell(o, carry):
        t = lax.rem(g_me + o, dp)
        pltpu.make_async_remote_copy(
            src_ref=side_ref, dst_ref=side_buf.at[g_me], send_sem=side_send, recv_sem=side_recv,
            device_id=(t, v_me), device_id_type=MESH).start()
        return carry

    lax.fori_loop(1, dp, tell, 0)
    relay(0)
    across(0)
    if chunks > 1:
        line(1, True)
    corner(0)
    others = side_buf.at[pl.ds(0, dp - 1)]
    pltpu.make_async_copy(others, others, side_recv).wait()
    pltpu.make_async_copy(others, others, side_send).wait()
    logit_ref[1] = jnp.zeros((vt, cols), jnp.float32)

    sub = lax.broadcasted_iota(jnp.int32, (8, cols), 0)
    groups = vt // 8

    def epilogue(g):
        s, i = g // tiles, g % tiles
        slot = g % 2
        c = chunk_of(s)
        ids = jnp.concatenate([side_buf[2 * c, 0:1, :], side_buf[2 * c + 1, 0:1, :]], axis=1).astype(jnp.int32)
        rel = ids - (me * (vt * tiles) + i * vt) - sub
        first = jnp.full((8, cols), i, jnp.int32) == 0
        m_old = jnp.where(first, LOW, m_ref[...])
        tops = [m_old] + [None] * 3
        for j in range(groups):
            val = logit_ref[slot, 8 * j:8 * j + 8, :]
            q = j % 4
            tops[q] = val if tops[q] is None else jnp.maximum(tops[q], val)
        m_new = functools.reduce(jnp.maximum, [t for t in tops if t is not None])
        sums = [jnp.where(first, 0.0, l_ref[...]) * jnp.exp(m_old - m_new), jnp.zeros((8, cols), jnp.float32)]
        picks = [jnp.where(first, 0.0, p_ref[...]), jnp.zeros((8, cols), jnp.float32)]
        for j in range(groups):
            val = logit_ref[slot, 8 * j:8 * j + 8, :]
            q = j % 2
            sums[q] = sums[q] + jnp.exp(val - m_new)
            picks[q] = picks[q] + jnp.where(rel == 8 * j, val, 0.0)
        m_ref[...] = m_new
        l_ref[...] = sums[0] + sums[1]
        p_ref[...] = picks[0] + picks[1]

    def finish(s):
        c = chunk_of(s)
        m, l, p = m_ref[...], l_ref[...], p_ref[...]
        peak = jnp.max(m, axis=0, keepdims=True)
        total = jnp.sum(l * jnp.exp(m - peak), axis=0, keepdims=True)
        pick = jnp.sum(p, axis=0, keepdims=True)
        pad = jnp.zeros((2, rows), jnp.float32)
        stat_ref[me, c] = jnp.concatenate(
            [peak[:, :rows], peak[:, rows:], total[:, :rows], total[:, rows:],
             pick[:, :rows], pick[:, rows:], pad], axis=0)

    def spread(s):
        c = chunk_of(s)
        mine = stat_ref.at[me, c]

        def one(o, carry):
            t = lax.rem(me + o, everyone)
            pltpu.make_async_remote_copy(
                src_ref=mine, dst_ref=mine, send_sem=stat_send, recv_sem=stat_recv,
                device_id=(lax.div(t, nv), lax.rem(t, nv)), device_id_type=MESH).start()
            return carry

        lax.fori_loop(1, everyone, one, 0)

    def step(g, carry):
        s, i = g // tiles, g % tiles
        slot = g % 2
        pl.when(s == 0)(lambda: wcopy(i).wait())
        pl.when(i == 0)(lambda: ready(s))

        def middle():
            relay(s + 1)
            pl.when(s + 2 < chunks)(lambda: line(s + 2, True))

        more = s + 1 < chunks
        pl.when((i == tiles // 3) & more)(middle)
        pl.when((i == (2 * tiles) // 3) & more)(lambda: across(s + 1))
        pl.when((i == tiles - 1) & more)(lambda: corner(s + 1))
        pl.when((i == 1) & (s > 0))(lambda: spread(s - 1))
        logit_ref[slot] = lax.dot_general(
            w_ref[i], h_ref[chunk_of(s)], (((1,), (1,)), ((), ())), preferred_element_type=jnp.float32)
        epilogue(jnp.where(g == 0, 1, g - 1))
        pl.when((i == 0) & (s > 0))(lambda: finish(s - 1))
        return carry

    last = chunks * tiles
    lax.fori_loop(0, last, step, 0)
    epilogue(last - 1)
    finish(chunks - 1)
    spread(chunks - 1)

    full, part = block(0, 0, 0, 0), block(0, 0, 0, 0, 0, half)

    def left(t, carry):
        for kind in (XA, XB, YA, YB, D0, D1):
            pltpu.make_async_copy(part, part, send.at[kind, t]).wait()
        for kind in (PL, PX, PY, PD):
            pltpu.make_async_copy(full, full, send.at[kind, t]).wait()
        pl.when(t > 0)(lambda: pltpu.make_async_copy(full, full, send.at[L, t]).wait())
        return carry

    lax.fori_loop(0, chunks, left, 0)
    rest = stat_ref.at[pl.ds(0, everyone - 1)]
    pltpu.make_async_copy(rest, rest, stat_recv).wait()
    pltpu.make_async_copy(rest, rest, stat_send).wait()

    loss_sum = jnp.zeros((1, rows), jnp.float32)
    count = jnp.zeros((1, rows), jnp.float32)
    for c in range(chunks):
        top = stat_ref[0, c]
        for d in range(1, everyone):
            top = jnp.maximum(top, stat_ref[d, c])
        total = jnp.zeros((2, rows), jnp.float32)
        pick = jnp.zeros((2, rows), jnp.float32)
        for d in range(everyone):
            t = stat_ref[d, c]
            total = total + t[2:4] * jnp.exp(t[0:2] - top[0:2])
            pick = pick + t[4:6]
        logp = pick - (top[0:2] + jnp.log(total))
        for r in range(2):
            g = 2 * c + r
            lp = logp[r:r + 1]
            mask, roll, adv = side_buf[g, 1:2, :], side_buf[g, 2:3, :], side_buf[g, 3:4, :]
            weight = jnp.minimum(jnp.exp(lp - roll), 2.0)
            loss_sum = loss_sum - mask * weight * adv * lp
            count = count + mask
            fin_ref[g, 0:1, :] = lp
            fin_ref[g, 1:2, :] = weight
    loss = jnp.sum(loss_sum, axis=1, keepdims=True) / jnp.maximum(jnp.sum(count, axis=1, keepdims=True), 1.0)
    out_ref[0:2, :] = fin_ref[g_me, 0:2, :]
    out_ref[2:8, :] = jnp.broadcast_to(loss, (6, rows))


def tile_rows(vocab_local):
    fits = [t for t in range(16, 1601, 16) if vocab_local % t == 0]
    return max(fits) if fits else 0


def fused_body(dp, nv, vt, hidden_states, head_weight, token_ids, response_mask, rollout_logprobs, advantages):
    rows, feats = hidden_states.shape
    vocab_local, width = head_weight.shape
    chunks, tiles = dp // 2, vocab_local // vt
    side = jnp.stack([token_ids.astype(jnp.float32), response_mask.astype(jnp.float32),
                      rollout_logprobs, advantages] + [jnp.zeros_like(advantages)] * 4)
    any_spec = pl.BlockSpec(memory_space=pl.ANY)
    vmem_spec = pl.BlockSpec(memory_space=pltpu.VMEM)
    dma = pltpu.SemaphoreType.DMA
    out = pl.pallas_call(
        functools.partial(kernel, dp, nv, rows, feats, vt, tiles),
        out_shape=jax.ShapeDtypeStruct((8, rows), jnp.float32),
        in_specs=[any_spec, any_spec, vmem_spec],
        out_specs=vmem_spec,
        scratch_shapes=[
            pltpu.VMEM((chunks, 2 * rows, width), jnp.bfloat16),
            pltpu.VMEM((tiles, vt, width), jnp.bfloat16),
            pltpu.VMEM((2, vt, 2 * rows), jnp.float32),
            pltpu.VMEM((8, 2 * rows), jnp.float32),
            pltpu.VMEM((8, 2 * rows), jnp.float32),
            pltpu.VMEM((8, 2 * rows), jnp.float32),
            pltpu.VMEM((dp * nv, chunks, 8, rows), jnp.float32),
            pltpu.VMEM((dp, 8, rows), jnp.float32),
            pltpu.VMEM((dp, 8, rows), jnp.float32),
            dma((11, chunks)), dma((11, chunks)), dma((tiles,)), dma, dma, dma, dma, dma,
        ],
        compiler_params=pltpu.CompilerParams(
            collective_id=0, has_side_effects=True, vmem_limit_bytes=VMEM_BYTES),
    )(hidden_states, head_weight, side)
    return out[0], out[1], out[2, 0]


def solution(mesh):
    placed = (P("dp", "vocab"), P(("dp", "vocab"), None), P("dp"), P("dp"), P("dp"), P("dp"))
    dp, nv = mesh.shape["dp"], mesh.shape["vocab"]

    def body(hidden_states, head_weight, *rest):
        rows, feats = hidden_states.shape
        vt = tile_rows(head_weight.shape[0])
        held = 2 * (head_weight.size + rows * dp * head_weight.shape[1]) + 16 * vt * rows
        fits = (dp % 2 == 0 and dp > 2 and nv == 4 and vt > 0 and rows == 128 and feats % 128 == 0
                and held < VMEM_BYTES - (8 << 20))
        if fits:
            return fused_body(dp, nv, vt, hidden_states, head_weight, *rest)
        return general_body(hidden_states, head_weight, *rest)

    return jax.shard_map(
        body, mesh=mesh, in_specs=placed, out_specs=(P("dp"), P("dp"), P()), check_vma=False
    )
```
